1024 devices in a mesh: gx: 128 (over x, z), gy: 8 (over y, core).
Axes of the slice: x: 4, y: 4, z: 32, core: 2. Of those that a mesh axis runs over, the one named last changes fastest.
Arguments:
- state: float32 [2097152, 128], P(('gx', 'gy')), may hold values from 0 to 1
- velocity: bfloat16 [3, 3, 2048, 128, 128], P(None, None, 'gx', 'gy'), may hold values from -3 to 3
- cells: int32 [3, 3, 2097152], P(None, None, ('gx', 'gy')), may hold values from -1 to 126, as said below
- slots: int32 [3, 2097152], P(None, ('gx', 'gy')), may hold values from 0 to 2047, as said below
- counts: int32 [3, 128, 8, 8], P(None, 'gx', 'gy'), may hold values from 0 to 64, as said below
Outputs:
- final_state: float32 [2097152, 128], P(('gx', 'gy'))
The draws below stay inside these ranges and needn't reach their ends.
Inputs may be any that keep to these rules, and one draw needn't show every extreme that they name: For every section and device the 2048 values of slots are a permutation of 0 to 2047. counts[s, i, j, r] equals counts[s, i', j', r xor 1] where (i', j') is the neighbour of (i, j) in direction r; some device sends exactly 64 in every section. cells[s, 0] lies in -1 to 15, cells[s, 1] in -1 to 15, cells[s, 2] in 0 to 126.
All inputs are finite; a program needn't handle non-finite values.
Results may differ from the reference program's by a relative error of at most 0.0003.
Values may be sent and summed in bfloat16 or wider, within the bound.
A program may use at most 32 MiB of HBM per device.

```python
import jax
import jax.numpy as jnp

CX = 16
CY = 16
NZ = 128
PART_DEV = 2048
CAP = 64
S = 128
SECTIONS = 3
NX = 2048
NY = 128
NPART = 2097152
N_GX = 128
N_GY = 8


def draw_counts(key, part):
    forward = jax.random.randint(key, (SECTIONS, N_GX, N_GY, 4), CAP // 4, CAP + 1)
    picks = jax.random.randint(jax.random.fold_in(key, 7), (SECTIONS,), 0, N_GX * N_GY)
    hot = (jnp.arange(N_GX * N_GY)[None, :] == picks[:, None]).reshape(SECTIONS, N_GX, N_GY)
    east = jnp.where(hot, CAP, forward[..., 0])
    north = forward[..., 1]
    rising = forward[..., 2]
    falling = forward[..., 3]
    table = jnp.stack([east, jnp.roll(east, 1, axis=1), north, jnp.roll(north, 1, axis=2), rising, jnp.roll(rising, (1, 1), axis=(1, 2)), falling, jnp.roll(falling, (1, -1), axis=(1, 2))], axis=-1)
    return table.astype(jnp.int32)


def draw_slots(key, part):
    scores = jax.random.randint(key, (SECTIONS, N_GX * N_GY, PART_DEV), 0, 2 ** 18)
    scores = scores * PART_DEV + jnp.arange(PART_DEV, dtype=jnp.int32)[None, None, :]
    order = jnp.argsort(scores, axis=-1, stable=True).astype(jnp.int32)
    return order.reshape(SECTIONS, N_GX * N_GY * PART_DEV)


def draw_cells(key, part):
    npart = N_GX * N_GY * PART_DEV
    cell_x = jax.random.randint(jax.random.fold_in(key, 1), (SECTIONS, npart), -1, CX)
    cell_y = jax.random.randint(jax.random.fold_in(key, 2), (SECTIONS, npart), -1, CY)
    cell_z = jax.random.randint(jax.random.fold_in(key, 3), (SECTIONS, npart), 0, NZ - 1)
    return jnp.stack([cell_x, cell_y, cell_z], axis=1).astype(jnp.int32)


def level_of(key, shape, split, low, top_value):
    gain = 1.0
    for position, parts in split:
        draws = jax.random.uniform(jax.random.fold_in(jax.random.fold_in(key, 6), position), (parts,), jnp.float32, low / len(split), top_value / len(split))
        gain = gain * jnp.repeat(jnp.exp(draws), shape[position] // parts).reshape((-1,) + (1,) * (len(shape) - 1 - position))
    return gain


def normal_values(own_key, dims, scale, reach, pieces=(), held_as=jnp.bfloat16):
    gain = level_of(own_key, dims, pieces, -0.22, 0.18) if pieces else 1.0
    array = jax.random.normal(own_key, dims, jnp.float32) * scale * gain
    return jnp.minimum(jnp.maximum(array, -reach), reach).astype(held_as)


def setup_inputs(seed: int = 0) -> dict:
    key_of = jax.random.split(jax.random.key(seed), 6)
    state = jnp.clip(1.0 * jax.random.uniform(key_of[0], (NPART, S), jnp.float32) ** level_of(key_of[0], (NPART, S), ((0, 1024),), -0.2, 0.2), 0.0, 1.0)
    velocity = normal_values(key_of[1], (SECTIONS, 3, NX, NY, NZ), 0.4, 3.0, ((2, 128), (3, 8)))
    cells = draw_cells(jax.random.fold_in(key_of[5], 71), 0)
    slots = draw_slots(jax.random.fold_in(key_of[5], 71), 0)
    counts = draw_counts(jax.random.fold_in(key_of[5], 71), 0)
    return dict(state=state, velocity=velocity, cells=cells, slots=slots, counts=counts)


GAMMA = (8.0 / 15.0, 5.0 / 12.0, 3.0 / 4.0)
ZETA = (0.0, -17.0 / 60.0, -5.0 / 12.0)
OFFSETS = ((1, 0), (-1, 0), (0, 1), (0, -1), (1, 1), (-1, -1), (1, -1), (-1, 1))
OPPOSITE = (1, 0, 3, 2, 5, 4, 7, 6)


def reference(state, velocity, cells, slots, counts):
    devices = N_GX * N_GY
    npart = devices * PART_DEV
    owner = jnp.arange(npart, dtype=jnp.int32) // PART_DEV
    row_i = owner // N_GY
    col_j = owner % N_GY
    lanes = jnp.arange(devices, dtype=jnp.int32)
    lane_i = lanes // N_GY
    lane_j = lanes % N_GY
    within = jnp.arange(CAP, dtype=jnp.int32)
    for section in range(SECTIONS):
        field = velocity[section]
        base_x = row_i * CX + cells[section, 0]
        base_y = col_j * CY + cells[section, 1]
        base_z = cells[section, 2]
        frac = state[:, 0:3]
        sampled = jnp.zeros((3, npart), jnp.float32)
        for a in (0, 1):
            for b in (0, 1):
                for c in (0, 1):
                    weight_x = frac[:, 0] if a else 1.0 - frac[:, 0]
                    weight_y = frac[:, 1] if b else 1.0 - frac[:, 1]
                    weight_z = frac[:, 2] if c else 1.0 - frac[:, 2]
                    index_x = (base_x + a) % NX
                    index_y = (base_y + b) % NY
                    values = field[:, index_x, index_y, base_z + c].astype(jnp.float32)
                    sampled = sampled + (weight_x * weight_y * weight_z)[None, :] * values
        speed = sampled.T
        moved = frac + GAMMA[section] * speed + ZETA[section] * state[:, 3:6]
        state = jnp.concatenate([moved, speed, state[:, 6:]], axis=1)
        order = slots[section].reshape(devices, PART_DEV)
        tally = counts[section].reshape(devices, 8)
        source = jnp.arange(npart, dtype=jnp.int32)
        for direction in range(8):
            off_x, off_y = OFFSETS[direction]
            back = OPPOSITE[direction]
            neighbour = ((lane_i + off_x) % N_GX) * N_GY + (lane_j + off_y) % N_GY
            far = neighbour[:, None] * PART_DEV + order[neighbour, back * CAP:(back + 1) * CAP]
            near = lanes[:, None] * PART_DEV + order[:, direction * CAP:(direction + 1) * CAP]
            picked = jnp.where(within[None, :] < tally[:, direction:direction + 1], far, near)
            source = source.at[near.reshape(-1)].set(picked.reshape(-1).astype(jnp.int32))
        state = state[source]
    return state
```

```python
import jax
import jax.numpy as jnp
from jax import lax
from jax.experimental import pallas as pl
from jax.experimental.pallas import tpu as pltpu
from jax.sharding import PartitionSpec as P

GAMMA = (8.0 / 15.0, 5.0 / 12.0, 3.0 / 4.0)
ZETA = (0.0, -17.0 / 60.0, -5.0 / 12.0)
OFFSETS = ((1, 0), (-1, 0), (0, 1), (0, -1), (1, 1), (-1, -1), (1, -1), (-1, 1))
CAP = 64
SLOTS = 2048
MOVE = 512
CHUNK = 512
F32 = jnp.float32
BF16 = jnp.bfloat16
I32 = jnp.int32
VMEM = pltpu.VMEM
SMEM = pltpu.SMEM
ANY = pl.ANY


def iota(shape, dim):
    return lax.broadcasted_iota(I32, shape, dim)


def lane_gather(x, index):
    return jnp.take_along_axis(x, index, axis=1, mode="promise_in_bounds")


def copy_rows(target, source, index, shift=0):
    def body(i, carry):
        for u in range(16):
            k = i * 16 + u
            target[pl.ds(k, 1), :] = source[pl.ds(index(k), 1), :]
        return carry

    lax.fori_loop(0, MOVE // 16, body, 0)


def prep_kernel(counts, leaving, slots, state, vel, pv, inv, ptr, dst, faces, corners, rows0, planes):
    for b in range(16):
        pv[:, b * 128 : (b + 1) * 128] = state[b * 128 : (b + 1) * 128, :].T[0:8, :]
    for j in range(9):
        planes[...] = vel[j * 256 : (j + 1) * 256, :].astype(F32)
        for side, y in ((0, 0), (1, 15)):
            faces[side, j] = planes[pl.ds(y, 16, stride=16), :].astype(BF16)
    for c in range(4):
        x, y = 15 * (c // 2), 15 * (c % 2)
        picked = [vel[j * 256 + x * 16 : j * 256 + x * 16 + 16, :].astype(F32)[y : y + 1, :] for j in range(9)]
        picked.append(jnp.zeros((7, 128), F32))
        corners[c] = jnp.concatenate(picked, axis=0).astype(BF16)
    loc = iota((16, 128), 0) * 128 + iota((16, 128), 1)
    lane = iota((1, 128), 1)
    row = iota((16, 128), 0)
    for s in range(3):
        heads = []
        tails = []
        for g in range(4):
            q = slots[s : s + 1, g * 128 : (g + 1) * 128]
            limit = jnp.where(lane < CAP, counts[s, 2 * g], counts[s, 2 * g + 1])
            valid = jnp.where(lane < CAP, lane, lane - CAP) < limit
            dst[s, g : g + 1, :] = jnp.where(valid, q, SLOTS)
            low = jnp.broadcast_to(q & 127, (8, 128))
            mine = jnp.broadcast_to(q >> 7, (16, 128)) == row
            found = jnp.concatenate([lane_gather(loc[0:8], low), lane_gather(loc[8:16], low)], axis=0)
            ptr[s, g : g + 1, :] = jnp.sum(jnp.where(mine, found, 0), axis=0, keepdims=True)
            place = (lane + g * 128) ^ CAP
            chosen = jnp.where(mine, jnp.where(valid, 1.0, 0.0), 0.0)
            upper = (place >> 5).astype(F32)
            lower = (place & 31).astype(F32)
            heads.append(jnp.concatenate([chosen, chosen * upper, chosen * lower], axis=0))
            tails.append(jnp.where(iota((128, 128), 0) == (q & 127), 1.0, 0.0))
        head = jnp.concatenate(heads, axis=1).astype(BF16)
        tail = jnp.concatenate(tails, axis=1).astype(BF16)
        table = lax.dot_general(head, tail, (((1,), (1,)), ((), ())), preferred_element_type=F32)
        value = (table[16:32] * 32.0 + table[32:48]).astype(I32)
        hit = table[0:16] > 0.5
        inv[s] = jnp.where(hit, value, -1)
        loc = jnp.where(hit, SLOTS + s * MOVE + (value ^ CAP), loc)
    copy_rows(rows0, state, lambda k: leaving[0, k])


def split(x):
    high = x.astype(BF16).astype(F32)
    return high, x - high


def step_kernel(
    ptr, pv0, inv, cells, slots, faces, corners, rows0, state, vel,
    pv_out, rows_out,
    pool, rows, landed, block, grid_v, halo_x, halo_y, halo_c, field, wx_table, sums, pv, out_pv, in_pv,
    local_sem, x_send, x_recv, y_send, y_recv, c_send, c_recv, r_send, r_recv, p_send, p_recv,
):
    me_x, me_y = lax.axis_index("gx"), lax.axis_index("gy")
    n_x, n_y = lax.axis_size("gx"), lax.axis_size("gy")

    def toward(r):
        dx, dy = OFFSETS[r]
        return (lax.rem(me_x + dx + n_x, n_x), lax.rem(me_y + dy + n_y, n_y))

    def remote(source, target, send, recv, r):
        return pltpu.make_async_remote_copy(
            src_ref=source, dst_ref=target, send_sem=send, recv_sem=recv,
            device_id=toward(r), device_id_type=pl.DeviceIdType.MESH,
        )

    load_vel = pltpu.make_async_copy(vel, block, local_sem.at[0])
    load_vel.start()
    load_state = pltpu.make_async_copy(state, pool.at[pl.ds(0, SLOTS)], local_sem.at[1])
    load_state.start()

    barrier = pltpu.get_barrier_semaphore()
    for r in range(8):
        pl.semaphore_signal(barrier, inc=1, device_id=toward(r), device_id_type=pl.DeviceIdType.MESH)
    pv[...] = pv0[...]
    load_vel.wait()
    for s in range(3):
        for k in range(3):
            own = block[s * 3 + k].reshape(256, 128)
            field[s, k * 256 : (k + 1) * 256, 0:128] = own
            field[s, k * 256 : (k + 1) * 256, 128:256] = own
    pl.semaphore_wait(barrier, 8)

    def rows_target(s, r):
        back = r ^ 1
        if s == 0:
            return pool.at[pl.ds(SLOTS + back * CAP, CAP)]
        return landed.at[s - 1, pl.ds(back * CAP, CAP)]

    def halo(s):
        part = pl.ds(s * 3, 3)
        copies = []
        for side, x, r in ((1, 0, 1), (0, 15, 0)):
            copies.append(remote(block.at[part, x], halo_x.at[side, part], x_send.at[s, side], x_recv.at[s, side], r))
        for side, edge, r in ((1, 0, 3), (0, 1, 2)):
            copies.append(remote(faces.at[edge, part], halo_y.at[side, part], y_send.at[s, side], y_recv.at[s, side], r))
        return copies

    corner_copies = [
        remote(corners.at[c], halo_c.at[3 - c], c_send.at[c], c_recv.at[3 - c], r)
        for c, r in ((0, 5), (1, 7), (2, 6), (3, 4))
    ]
    halos = [halo(s) for s in range(3)]
    row_copies = [
        [
            remote((rows0 if s == 0 else rows.at[s - 1]).at[pl.ds(r * CAP, CAP)], rows_target(s, r), r_send.at[s, r], r_recv.at[s, r ^ 1], r)
            for r in range(8)
        ]
        for s in range(3)
    ]
    pv_copies = [
        [remote(out_pv.at[s, r // 2], in_pv.at[s, r ^ 1], p_send.at[s, r], p_recv.at[s, r ^ 1], r) for r in range(8)]
        for s in range(3)
    ]
    for copy in halos[0] + corner_copies:
        copy.start()
    for copy in row_copies[0]:
        copy.start()
    for copy in halos[1] + halos[2]:
        copy.start()

    def both(target, value):
        target[:, 0:128] = value
        target[:, 128:256] = value

    def place_halo(s):
        for copy in halos[s]:
            copy.wait_recv()
        for side in range(2):
            both(field.at[s, pl.ds(768 + side * 48, 48)], halo_x[side, s * 3 : s * 3 + 3].reshape(48, 128))
            both(field.at[s, pl.ds(864 + side * 48, 48)], halo_y[side, s * 3 : s * 3 + 3].reshape(48, 128))
        for c in range(4):
            both(field.at[s, pl.ds(960 + c * 16, 16)], halo_c[c])

    def interpolate(s):
        def chunk(i, carry):
            at = pl.ds(pl.multiple_of(i * CHUNK, CHUNK), CHUNK)
            fx, fy, fz = pv[0:1, at], pv[1:2, at], pv[2:3, at]
            cx, cy, cz = cells[s, 0:1, at], cells[s, 1:2, at], cells[s, 2:3, at]
            near_hi, near_lo = split(1.0 - fz)
            far_hi, far_lo = split(fz)
            level = iota((128, CHUNK), 0)
            near = level == cz
            far = level == cz + 1
            weight = jnp.concatenate(
                [
                    jnp.where(near, near_hi, jnp.where(far, far_hi, 0.0)).astype(BF16),
                    jnp.where(near, near_lo, jnp.where(far, far_lo, 0.0)).astype(BF16),
                ],
                axis=0,
            )
            sums[...] = jnp.dot(field[s], weight, preferred_element_type=F32)
            spot = iota((16, CHUNK), 0)
            wx = jnp.where(spot == cx, 1.0 - fx, jnp.where(spot == cx + 1, fx, 0.0))
            wy = jnp.where(spot == cy, 1.0 - fy, jnp.where(spot == cy + 1, fy, 0.0))
            wx_table[...] = wx
            wx_low = jnp.where(cx == -1, 1.0 - fx, 0.0)
            wx_high = jnp.where(cx == 15, fx, 0.0)
            wy_low = jnp.where(cy == -1, 1.0 - fy, 0.0)
            wy_high = jnp.where(cy == 15, fy, 0.0)
            corner = jnp.zeros((16, CHUNK), F32)
            for c, w in enumerate((wx_low * wy_low, wx_low * wy_high, wx_high * wy_low, wx_high * wy_high)):
                corner = corner + sums[960 + c * 16 : 976 + c * 16, :] * w
            old = pv[:, at]
            new = []
            speeds = []
            for k in range(3):
                along = sums[768 + k * 16 : 784 + k * 16, :] * wx_low + sums[816 + k * 16 : 832 + k * 16, :] * wx_high
                for x in range(16):
                    along = along + sums[k * 256 + x * 16 : k * 256 + x * 16 + 16, :] * wx_table[x : x + 1, :]
                edge = sums[864 + k * 16 : 880 + k * 16, :] * wy_low + sums[912 + k * 16 : 928 + k * 16, :] * wy_high
                total = along * wy + edge * wx + jnp.where(spot == s * 3 + k, corner, 0.0)
                speed = jnp.sum(total, axis=0, keepdims=True)
                speeds.append(speed)
                new.append(old[k : k + 1] + GAMMA[s] * speed + ZETA[s] * old[3 + k : 4 + k])
            for k in range(3):
                pv[k : k + 1, at] = new[k]
                pv[3 + k : 4 + k, at] = speeds[k]
            return carry

        lax.fori_loop(0, SLOTS // CHUNK, chunk, 0)

    def collect(s):
        for g in range(4):
            q = slots[s : s + 1, g * 128 : (g + 1) * 128]
            low = jnp.broadcast_to(q & 127, (8, 128))
            high = jnp.broadcast_to(q >> 7, (8, 128))
            picked = jnp.zeros((8, 128), F32)
            for h in range(16):
                picked = jnp.where(high == h, lane_gather(pv[:, h * 128 : (h + 1) * 128], low), picked)
            out_pv[s, g] = picked

    def deliver(s):
        lane = iota((8, 128), 1)
        came = [jnp.where(lane < CAP, in_pv[s, 2 * g + 1], in_pv[s, 2 * g]) for g in range(4)]
        for h in range(16):
            at = slice(h * 128, (h + 1) * 128)
            source = jnp.broadcast_to(inv[s, h : h + 1, :], (8, 128))
            low = source & 127
            high = source >> 7
            value = pv[:, at]
            for g in range(4):
                value = jnp.where(high == g, lane_gather(came[g], low), value)
            pv[:, at] = value

    for copy in corner_copies:
        copy.wait_recv()
    for s in range(3):
        place_halo(s)
        interpolate(s)
        collect(s)
        for copy in pv_copies[s]:
            copy.start()
        if s == 0:
            load_state.wait()
        for copy in row_copies[s]:
            copy.wait_recv()
        if s == 1:
            pool[SLOTS + MOVE : SLOTS + 2 * MOVE, :] = landed[0]
        if s < 2:
            copy_rows(rows.at[s], pool, lambda k: ptr[s + 1, k])
            for copy in row_copies[s + 1]:
                copy.start()
        else:
            out_a = pltpu.make_async_copy(pool.at[pl.ds(SLOTS, 2 * MOVE)], rows_out.at[pl.ds(0, 2 * MOVE)], local_sem.at[2])
            out_a.start()
            out_b = pltpu.make_async_copy(landed.at[1], rows_out.at[pl.ds(2 * MOVE, MOVE)], local_sem.at[3])
            out_b.start()
        for copy in pv_copies[s]:
            copy.wait_recv()
        deliver(s)
    pv_out[...] = pv[...]
    out_a.wait()
    out_b.wait()
    for copies in halos + [corner_copies] + row_copies + pv_copies:
        for copy in copies:
            copy.wait_send()


def finish_kernel(dst, state, rows, pv, out, held, sem):
    load = pltpu.make_async_copy(state, held.at[pl.ds(0, SLOTS)], sem)
    load.start()
    load.wait()
    for s in range(3):
        def body(i, carry):
            for u in range(16):
                k = i * 16 + u
                held[pl.ds(dst[s, k], 1), :] = rows[pl.ds(s * MOVE + k, 1), :]
            return carry

        lax.fori_loop(0, MOVE // 16, body, 0)
    for b in range(16):
        held[b * 128 : (b + 1) * 128, 0:8] = pv[:, b * 128 : (b + 1) * 128].T
    store = pltpu.make_async_copy(held.at[pl.ds(0, SLOTS)], out, sem)
    store.start()
    store.wait()


def whole(space):
    return pl.BlockSpec(memory_space=space)


def shape(dims, dtype):
    return jax.ShapeDtypeStruct(dims, dtype)


def local(state, velocity, cells, slots, counts):
    flat = velocity.reshape(2304, 128)
    pv, inv, ptr, dst, faces, corners, rows0 = pl.pallas_call(
        prep_kernel,
        grid=(1,),
        out_shape=(
            shape((8, SLOTS), F32), shape((3, 16, 128), I32), shape((3, 4, 128), I32), shape((3, 4, 128), I32),
            shape((2, 9, 16, 128), BF16), shape((4, 16, 128), BF16), shape((MOVE, 128), F32),
        ),
        in_specs=[
            whole(SMEM),
            pl.BlockSpec((3, MOVE), lambda i: (0, 0), memory_space=SMEM),
            pl.BlockSpec((3, MOVE), lambda i: (0, 0)),
            whole(VMEM),
            whole(VMEM),
        ],
        out_specs=[whole(VMEM)] * 7,
        scratch_shapes=[VMEM((256, 128), F32)],
        name="prep",
    )(counts.reshape(3, 8), slots, slots, state, flat)

    dma = pltpu.SemaphoreType.DMA
    pv, rows = pl.pallas_call(
        step_kernel,
        out_shape=(shape((8, SLOTS), F32), shape((3 * MOVE, 128), F32)),
        in_specs=[whole(SMEM)] + [whole(VMEM)] * 7 + [whole(ANY)] * 2,
        out_specs=[whole(VMEM), whole(ANY)],
        scratch_shapes=[
            VMEM((SLOTS + 2 * MOVE, 128), F32),
            VMEM((2, MOVE, 128), F32),
            VMEM((2, MOVE, 128), F32),
            VMEM((9, 16, 16, 128), BF16),
            VMEM((8, 128), F32),
            VMEM((2, 9, 16, 128), BF16),
            VMEM((2, 9, 16, 128), BF16),
            VMEM((4, 16, 128), BF16),
            VMEM((3, 1024, 256), BF16),
            VMEM((16, CHUNK), F32),
            VMEM((1024, CHUNK), F32),
            VMEM((8, SLOTS), F32),
            VMEM((3, 4, 8, 128), F32),
            VMEM((3, 8, 8, 128), F32),
            dma((4,)),
            dma((3, 2)), dma((3, 2)), dma((3, 2)), dma((3, 2)),
            dma((4,)), dma((4,)),
            dma((3, 8)), dma((3, 8)), dma((3, 8)), dma((3, 8)),
        ],
        compiler_params=pltpu.CompilerParams(collective_id=0, has_side_effects=True),
        name="step",
    )(ptr.reshape(3, MOVE), pv, inv, cells, slots, faces, corners, rows0, state, velocity.reshape(9, 16, 16, 128))

    return pl.pallas_call(
        finish_kernel,
        out_shape=shape((SLOTS, 128), F32),
        in_specs=[whole(SMEM), whole(ANY), whole(VMEM), whole(VMEM)],
        out_specs=whole(ANY),
        scratch_shapes=[VMEM((SLOTS + 8, 128), F32), dma],
        name="finish",
    )(dst.reshape(3, MOVE), state, rows, pv)


def solution(mesh):
    return jax.shard_map(
        local,
        mesh=mesh,
        in_specs=(
            P(("gx", "gy"), None),
            P(None, None, "gx", "gy", None),
            P(None, None, ("gx", "gy")),
            P(None, ("gx", "gy")),
            P(None, "gx", "gy", None),
        ),
        out_specs=P(("gx", "gy"), None),
        check_vma=False,
    )
```

```python
import jax
import jax.numpy as jnp
from jax import lax
from jax.experimental import pallas as pl
from jax.experimental.pallas import tpu as pltpu
from jax.sharding import PartitionSpec as P

GAMMA = (8.0 / 15.0, 5.0 / 12.0, 3.0 / 4.0)
ZETA = (0.0, -17.0 / 60.0, -5.0 / 12.0)
OFFSETS = ((1, 0), (-1, 0), (0, 1), (0, -1), (1, 1), (-1, -1), (1, -1), (-1, 1))
CAP = 64
SLOTS = 2048
MOVE = 512
CHUNK = 512
F32 = jnp.float32
BF16 = jnp.bfloat16
I32 = jnp.int32
VMEM = pltpu.VMEM
SMEM = pltpu.SMEM
ANY = pl.ANY


def iota(shape, dim):
    return lax.broadcasted_iota(I32, shape, dim)


def lane_gather(x, index):
    return jnp.take_along_axis(x, index, axis=1, mode="promise_in_bounds")


def copy_rows(target, source, index):
    def body(g, carry):
        for u in range(128):
            target[pl.ds(g * 128 + u, 1), :] = source[pl.ds(index(g, u), 1), :]
        return carry

    lax.fori_loop(0, MOVE // 128, body, 0)


def edges(block, y):
    picked = [block[j, x].astype(F32)[y : y + 1, :] for j in range(9) for x in range(16)]
    return jnp.concatenate(picked, axis=0).astype(BF16).reshape(9, 16, 128)


def corner_rows(block, c):
    x, y = 15 * (c // 2), 15 * (c % 2)
    picked = [block[j, x].astype(F32)[y : y + 1, :] for j in range(9)]
    picked.append(jnp.zeros((7, 128), F32))
    return jnp.concatenate(picked, axis=0).astype(BF16)


def rows_dot(a, b):
    return lax.dot_general(a, b, (((1,), (1,)), ((), ())), preferred_element_type=F32)


def tables(counts, slots, ptr, dst, home, tail, filled):
    lane = iota((1, 128), 1)
    across = iota((8, 128), 1)
    down = iota((8, 128), 0)
    leaving = [[slots[s : s + 1, g * 128 : (g + 1) * 128] for g in range(4)] for s in range(3)]
    found = {}
    for s in range(3):
        for g in range(4):
            q = leaving[s][g]
            limit = jnp.where(lane < CAP, counts[s, 0, 0, 2 * g], counts[s, 0, 0, 2 * g + 1])
            valid = jnp.where(lane < CAP, lane, lane - CAP) < limit
            dst[s * 4 + g : s * 4 + g + 1, :] = jnp.where(valid, q, SLOTS)
            code = jnp.broadcast_to(jnp.where(valid, q, -1), (8, 128))
            swapped = lane_gather(code, across ^ CAP)[0:1, :]
            at = slice(g * 128, (g + 1) * 128)
            home[s : s + 1, at] = swapped >> 7
            tail[s, :, at] = jnp.where(iota((128, 128), 0) == (swapped & 127), 1.0, 0.0).astype(BF16)
            if s < 2:
                for j in range(16):
                    column = lane_gather(code, down + 8 * j)
                    place = down + (SLOTS + s * MOVE + g * 128 + 8 * j)
                    for later in range(s + 1, 3):
                        for f in range(4):
                            hit = jnp.where(column == leaving[later][f], place, 0)
                            key = (s, later, f)
                            found[key] = found[key] + hit if key in found else hit
        head = jnp.where(iota((16, MOVE), 0) == home[s : s + 1, :], 1.0, 0.0).astype(BF16)
        filled[s] = rows_dot(head, tail[s])
    for f in range(4):
        total = {key: jnp.sum(found[key + (f,)], axis=0, keepdims=True) for key in ((0, 1), (0, 2), (1, 2))}
        ptr[f : f + 1, :] = jnp.where(total[0, 1] > 0, total[0, 1], leaving[1][f])
        early = jnp.where(total[0, 2] > 0, total[0, 2], leaving[2][f])
        ptr[4 + f : 5 + f, :] = jnp.where(total[1, 2] > 0, total[1, 2], early)


def split(x):
    high = x.astype(BF16).astype(F32)
    return high, x - high


def step_kernel(
    counts, cells_h, slots_h, state, vel,
    pv_out, rows_out, dst,
    pool, rows, landed, block, faces, corners, halo_x, halo_y, halo_c, field, wx_table, sums, pv, out_pv, in_pv,
    cells, slots, home, tail, filled, ptr, first, later,
    local_sem, x_send, x_recv, y_send, y_recv, c_send, c_recv, r_send, r_recv, p_send, p_recv,
):
    me_x, me_y = lax.axis_index("gx"), lax.axis_index("gy")
    n_x, n_y = lax.axis_size("gx"), lax.axis_size("gy")

    def toward(r):
        dx, dy = OFFSETS[r]
        return (lax.rem(me_x + dx + n_x, n_x), lax.rem(me_y + dy + n_y, n_y))

    def remote(source, target, send, recv, r):
        return pltpu.make_async_remote_copy(
            src_ref=source, dst_ref=target, send_sem=send, recv_sem=recv,
            device_id=toward(r), device_id_type=pl.DeviceIdType.MESH,
        )

    load_vel = pltpu.make_async_copy(vel, block, local_sem.at[0])
    load_first = pltpu.make_async_copy(slots_h.at[:, pl.ds(0, MOVE)], first, local_sem.at[4])
    load_state = pltpu.make_async_copy(state, pool.at[pl.ds(0, SLOTS)], local_sem.at[1])
    load_slots = pltpu.make_async_copy(slots_h.at[:, pl.ds(0, MOVE)], slots, local_sem.at[5])
    load_cells = pltpu.make_async_copy(cells_h, cells, local_sem.at[6])
    for load in (load_vel, load_first, load_state, load_slots, load_cells):
        load.start()

    barrier = pltpu.get_barrier_semaphore()
    for r in range(8):
        pl.semaphore_signal(barrier, inc=1, device_id=toward(r), device_id_type=pl.DeviceIdType.MESH)
    load_vel.wait()
    faces[0] = edges(block, 0)
    faces[1] = edges(block, 15)
    for c in range(4):
        corners[c] = corner_rows(block, c)
    pl.semaphore_wait(barrier, 8)

    def rows_target(s, r):
        return landed.at[s, pl.ds((r ^ 1) * CAP, CAP)]

    def halo(s):
        part = pl.ds(s * 3, 3)
        copies = []
        for side, x, r in ((1, 0, 1), (0, 15, 0)):
            copies.append(remote(block.at[part, x], halo_x.at[side, part], x_send.at[s, side], x_recv.at[s, side], r))
        for side, edge, r in ((1, 0, 3), (0, 1, 2)):
            copies.append(remote(faces.at[edge, part], halo_y.at[side, part], y_send.at[s, side], y_recv.at[s, side], r))
        return copies

    corner_copies = [
        remote(corners.at[c], halo_c.at[3 - c], c_send.at[c], c_recv.at[3 - c], r)
        for c, r in ((0, 5), (1, 7), (2, 6), (3, 4))
    ]
    halos = [halo(s) for s in range(3)]
    row_copies = [
        [
            remote(rows.at[s, pl.ds(r * CAP, CAP)], rows_target(s, r), r_send.at[s, r], r_recv.at[s, r ^ 1], r)
            for r in range(8)
        ]
        for s in range(3)
    ]
    pv_copies = [
        [remote(out_pv.at[s, r // 2], in_pv.at[s, r ^ 1], p_send.at[s, r], p_recv.at[s, r ^ 1], r) for r in range(8)]
        for s in range(3)
    ]
    for copy in halos[0] + corner_copies:
        copy.start()
    load_first.wait()
    load_state.wait()
    copy_rows(rows.at[0], pool, lambda g, u: first[0, g * 128 + u])
    for copy in row_copies[0]:
        copy.start()
    for copy in halos[1] + halos[2]:
        copy.start()
    for b in range(16):
        pv[:, b * 128 : (b + 1) * 128] = pool[b * 128 : (b + 1) * 128, :].T[0:8, :]
    load_slots.wait()
    tables(counts, slots, ptr, dst, home, tail, filled)
    load_later = pltpu.make_async_copy(ptr, later, local_sem.at[7])
    load_later.start()
    for s in range(3):
        for k in range(3):
            own = block[s * 3 + k].reshape(256, 128)
            field[s, k * 256 : (k + 1) * 256, 0:128] = own
            field[s, k * 256 : (k + 1) * 256, 128:256] = own
    load_cells.wait()
    load_later.wait()

    def both(target, value):
        target[:, 0:128] = value
        target[:, 128:256] = value

    def place_halo(s):
        for copy in halos[s]:
            copy.wait_recv()
        for side in range(2):
            both(field.at[s, pl.ds(768 + side * 48, 48)], halo_x[side, s * 3 : s * 3 + 3].reshape(48, 128))
            both(field.at[s, pl.ds(864 + side * 48, 48)], halo_y[side, s * 3 : s * 3 + 3].reshape(48, 128))
        for c in range(4):
            both(field.at[s, pl.ds(960 + c * 16, 16)], halo_c[c])

    def interpolate(s):
        def chunk(i, carry):
            at = pl.ds(pl.multiple_of(i * CHUNK, CHUNK), CHUNK)
            fx, fy, fz = pv[0:1, at], pv[1:2, at], pv[2:3, at]
            cx, cy, cz = cells[s, 0:1, at], cells[s, 1:2, at], cells[s, 2:3, at]
            near_hi, near_lo = split(1.0 - fz)
            far_hi, far_lo = split(fz)
            level = iota((128, CHUNK), 0)
            near = level == cz
            far = level == cz + 1
            weight = jnp.concatenate(
                [
                    jnp.where(near, near_hi, jnp.where(far, far_hi, 0.0)).astype(BF16),
                    jnp.where(near, near_lo, jnp.where(far, far_lo, 0.0)).astype(BF16),
                ],
                axis=0,
            )
            sums[...] = jnp.dot(field[s], weight, preferred_element_type=F32)
            spot = iota((16, CHUNK), 0)
            wx = jnp.where(spot == cx, 1.0 - fx, jnp.where(spot == cx + 1, fx, 0.0))
            wy = jnp.where(spot == cy, 1.0 - fy, jnp.where(spot == cy + 1, fy, 0.0))
            wx_table[...] = wx
            wx_low = jnp.where(cx == -1, 1.0 - fx, 0.0)
            wx_high = jnp.where(cx == 15, fx, 0.0)
            wy_low = jnp.where(cy == -1, 1.0 - fy, 0.0)
            wy_high = jnp.where(cy == 15, fy, 0.0)
            corner = jnp.zeros((16, CHUNK), F32)
            for c, w in enumerate((wx_low * wy_low, wx_low * wy_high, wx_high * wy_low, wx_high * wy_high)):
                corner = corner + sums[960 + c * 16 : 976 + c * 16, :] * w
            old = pv[:, at]
            new = []
            speeds = []
            for k in range(3):
                along = sums[768 + k * 16 : 784 + k * 16, :] * wx_low + sums[816 + k * 16 : 832 + k * 16, :] * wx_high
                for x in range(16):
                    along = along + sums[k * 256 + x * 16 : k * 256 + x * 16 + 16, :] * wx_table[x : x + 1, :]
                edge = sums[864 + k * 16 : 880 + k * 16, :] * wy_low + sums[912 + k * 16 : 928 + k * 16, :] * wy_high
                total = along * wy + edge * wx + jnp.where(spot == s * 3 + k, corner, 0.0)
                speed = jnp.sum(total, axis=0, keepdims=True)
                speeds.append(speed)
                new.append(old[k : k + 1] + GAMMA[s] * speed + ZETA[s] * old[3 + k : 4 + k])
            for k in range(3):
                pv[k : k + 1, at] = new[k]
                pv[3 + k : 4 + k, at] = speeds[k]
            return carry

        lax.fori_loop(0, SLOTS // CHUNK, chunk, 0)

    def collect(s):
        for g in range(4):
            q = slots[s : s + 1, g * 128 : (g + 1) * 128]
            low = jnp.broadcast_to(q & 127, (8, 128))
            high = jnp.broadcast_to(q >> 7, (8, 128))
            picked = jnp.zeros((8, 128), F32)
            for h in range(16):
                picked = jnp.where(high == h, lane_gather(pv[:, h * 128 : (h + 1) * 128], low), picked)
            out_pv[s, g] = picked

    def deliver(s):
        lane = iota((8, 128), 1)
        came = [jnp.where(lane < CAP, in_pv[s, 2 * g + 1], in_pv[s, 2 * g]) for g in range(4)]
        value = jnp.concatenate(came, axis=1)
        high, rest = split(value)
        middle, low = split(rest)
        to = home[s : s + 1, :]
        parts = [jnp.where(to == h, part, 0.0).astype(BF16) for part in (high, middle, low) for h in range(16)]
        spread = rows_dot(jnp.concatenate(parts, axis=0), tail[s])
        for h in range(16):
            at = slice(h * 128, (h + 1) * 128)
            r = h * 8
            new = spread[r : r + 8] + spread[128 + r : 136 + r] + spread[256 + r : 264 + r]
            pv[:, at] = jnp.where(filled[s, h : h + 1, :] > 0.5, new, pv[:, at])

    for copy in corner_copies:
        copy.wait_recv()
    stores = []
    for s in range(3):
        place_halo(s)
        interpolate(s)
        collect(s)
        for copy in pv_copies[s]:
            copy.start()
        for copy in row_copies[s]:
            copy.wait_recv()
        store = pltpu.make_async_copy(landed.at[s], rows_out.at[pl.ds(s * MOVE, MOVE)], local_sem.at[8 + s])
        store.start()
        stores.append(store)
        if s < 2:
            pool[SLOTS + s * MOVE : SLOTS + (s + 1) * MOVE, :] = landed[s]
            copy_rows(rows.at[s + 1], pool, lambda g, u: later[s * 4 + g, u])
            for copy in row_copies[s + 1]:
                copy.start()
        for copy in pv_copies[s]:
            copy.wait_recv()
        deliver(s)
    pv_out[...] = pv[...]
    for store in stores:
        store.wait()
    for copies in halos + [corner_copies] + row_copies + pv_copies:
        for copy in copies:
            copy.wait_send()


def finish_kernel(dst_h, state, rows_h, pv_h, out, held, rows, pv, dst, sem, out_sem):
    loads = [
        pltpu.make_async_copy(state, held.at[pl.ds(0, SLOTS)], sem.at[0]),
        pltpu.make_async_copy(dst_h, dst, sem.at[1]),
        pltpu.make_async_copy(rows_h, rows, sem.at[2]),
        pltpu.make_async_copy(pv_h, pv, sem.at[3]),
    ]
    for load in loads:
        load.start()
    for load in loads:
        load.wait()

    def body(g, carry):
        for u in range(128):
            held[pl.ds(dst[g, u], 1), :] = rows[pl.ds(g * 128 + u, 1), :]
        return carry

    lax.fori_loop(0, 12, body, 0)
    stores = []
    for c in range(4):
        for b in range(c * 4, c * 4 + 4):
            held[b * 128 : (b + 1) * 128, 0:8] = pv[:, b * 128 : (b + 1) * 128].T
        part = pl.ds(c * 512, 512)
        stores.append(pltpu.make_async_copy(held.at[part], out.at[part], out_sem.at[c]))
        stores[-1].start()
    for store in stores:
        store.wait()


def whole(space):
    return pl.BlockSpec(memory_space=space)


def shape(dims, dtype):
    return jax.ShapeDtypeStruct(dims, dtype)


def local(state, velocity, cells, slots, counts):
    dma = pltpu.SemaphoreType.DMA
    pv, rows, dst = pl.pallas_call(
        step_kernel,
        out_shape=(shape((8, SLOTS), F32), shape((3 * MOVE, 128), F32), shape((12, 128), I32)),
        in_specs=[whole(SMEM)] + [whole(ANY)] * 4,
        out_specs=[whole(VMEM), whole(ANY), whole(VMEM)],
        scratch_shapes=[
            VMEM((SLOTS + 2 * MOVE, 128), F32),
            VMEM((3, MOVE, 128), F32),
            VMEM((3, MOVE, 128), F32),
            VMEM((9, 16, 16, 128), BF16),
            VMEM((2, 9, 16, 128), BF16),
            VMEM((4, 16, 128), BF16),
            VMEM((2, 9, 16, 128), BF16),
            VMEM((2, 9, 16, 128), BF16),
            VMEM((4, 16, 128), BF16),
            VMEM((3, 1024, 256), BF16),
            VMEM((16, CHUNK), F32),
            VMEM((1024, CHUNK), F32),
            VMEM((8, SLOTS), F32),
            VMEM((3, 4, 8, 128), F32),
            VMEM((3, 8, 8, 128), F32),
            VMEM((3, 3, SLOTS), I32),
            VMEM((3, MOVE), I32),
            VMEM((3, MOVE), I32),
            VMEM((3, 128, MOVE), BF16),
            VMEM((3, 16, 128), F32),
            VMEM((8, 128), I32),
            SMEM((3, MOVE), I32),
            SMEM((8, 128), I32),
            dma((11,)),
            dma((3, 2)), dma((3, 2)), dma((3, 2)), dma((3, 2)),
            dma((4,)), dma((4,)),
            dma((3, 8)), dma((3, 8)), dma((3, 8)), dma((3, 8)),
        ],
        compiler_params=pltpu.CompilerParams(collective_id=0, has_side_effects=True),
        name="step",
    )(counts, cells, slots, state, velocity.reshape(9, 16, 16, 128))

    return pl.pallas_call(
        finish_kernel,
        out_shape=shape((SLOTS, 128), F32),
        in_specs=[whole(ANY)] * 4,
        out_specs=whole(ANY),
        scratch_shapes=[
            VMEM((SLOTS + 8, 128), F32),
            VMEM((3 * MOVE, 128), F32),
            VMEM((8, SLOTS), F32),
            SMEM((12, 128), I32),
            dma((4,)),
            dma((4,)),
        ],
        name="finish",
    )(dst, state, rows, pv)


def solution(mesh):
    return jax.shard_map(
        local,
        mesh=mesh,
        in_specs=(
            P(("gx", "gy"), None),
            P(None, None, "gx", "gy", None),
            P(None, None, ("gx", "gy")),
            P(None, ("gx", "gy")),
            P(None, "gx", "gy", None),
        ),
        out_specs=P(("gx", "gy"), None),
        check_vma=False,
    )
```

```python
import jax
import jax.numpy as jnp
from jax import lax
from jax.experimental import pallas as pl
from jax.experimental.pallas import tpu as pltpu
from jax.sharding import PartitionSpec as P

GAMMA = (8.0 / 15.0, 5.0 / 12.0, 3.0 / 4.0)
ZETA = (0.0, -17.0 / 60.0, -5.0 / 12.0)
OFFSETS = ((1, 0), (-1, 0), (0, 1), (0, -1), (1, 1), (-1, -1), (1, -1), (-1, 1))
CAP = 64
SLOTS = 2048
MOVE = 512
CHUNK = 512
F32 = jnp.float32
BF16 = jnp.bfloat16
I32 = jnp.int32
VMEM = pltpu.VMEM
SMEM = pltpu.SMEM
ANY = pl.ANY


def iota(shape, dim):
    return lax.broadcasted_iota(I32, shape, dim)


def lane_gather(x, index):
    return jnp.take_along_axis(x, index, axis=1, mode="promise_in_bounds")


def copy_rows(target, source, index, copies):
    def body(g, carry):
        for u in range(128):
            target[pl.ds(g * 128 + u, 1), :] = source[pl.ds(index(g, u), 1), :]
        return carry

    for half in range(2):
        lax.fori_loop(half * 2, half * 2 + 2, body, 0)
        for r in range(half * 4, half * 4 + 4):
            copies[r].start()


def edges(block, y):
    picked = [block[j, x].astype(F32)[y : y + 1, :] for j in range(9) for x in range(16)]
    return jnp.concatenate(picked, axis=0).astype(BF16).reshape(9, 16, 128)


def corner_rows(block, c):
    x, y = 15 * (c // 2), 15 * (c % 2)
    picked = [block[j, x].astype(F32)[y : y + 1, :] for j in range(9)]
    picked.append(jnp.zeros((7, 128), F32))
    return jnp.concatenate(picked, axis=0).astype(BF16)


def rows_dot(a, b):
    return lax.dot_general(a, b, (((1,), (1,)), ((), ())), preferred_element_type=F32)


def tables(counts, slots, ptr, dst, home, tail, filled):
    lane = iota((1, 128), 1)
    across = iota((8, 128), 1)
    down = iota((8, 128), 0)
    leaving = [[slots[s : s + 1, g * 128 : (g + 1) * 128] for g in range(4)] for s in range(3)]
    found = {}
    for s in range(3):
        for g in range(4):
            q = leaving[s][g]
            limit = jnp.where(lane < CAP, counts[s, 0, 0, 2 * g], counts[s, 0, 0, 2 * g + 1])
            valid = jnp.where(lane < CAP, lane, lane - CAP) < limit
            dst[s * 4 + g : s * 4 + g + 1, :] = jnp.where(valid, q, SLOTS)
            code = jnp.broadcast_to(jnp.where(valid, q, -1), (8, 128))
            swapped = lane_gather(code, across ^ CAP)[0:1, :]
            at = slice(g * 128, (g + 1) * 128)
            home[s : s + 1, at] = swapped >> 7
            tail[s, :, at] = jnp.where(iota((128, 128), 0) == (swapped & 127), 1.0, 0.0).astype(BF16)
            if s < 2:
                for j in range(16):
                    column = lane_gather(code, down + 8 * j)
                    place = down + (SLOTS + s * MOVE + g * 128 + 8 * j)
                    for later in range(s + 1, 3):
                        for f in range(4):
                            hit = jnp.where(column == leaving[later][f], place, 0)
                            key = (s, later, f)
                            found[key] = found[key] + hit if key in found else hit
        head = jnp.where(iota((16, MOVE), 0) == home[s : s + 1, :], 1.0, 0.0).astype(BF16)
        filled[s] = rows_dot(head, tail[s])
    for f in range(4):
        total = {key: jnp.sum(found[key + (f,)], axis=0, keepdims=True) for key in ((0, 1), (0, 2), (1, 2))}
        ptr[f : f + 1, :] = jnp.where(total[0, 1] > 0, total[0, 1], leaving[1][f])
        early = jnp.where(total[0, 2] > 0, total[0, 2], leaving[2][f])
        ptr[4 + f : 5 + f, :] = jnp.where(total[1, 2] > 0, total[1, 2], early)


def split(x):
    high = x.astype(BF16).astype(F32)
    return high, x - high


def step_kernel(
    counts, cells_h, slots_h, state, vel,
    pv_out, rows_out, dst,
    pool, rows, landed, block, faces, corners, halo_x, halo_y, halo_c, field, wx_table, sums, pv, out_pv, in_pv,
    cells, away, slots, home, tail, filled, ptr, first, later,
    local_sem, x_send, x_recv, y_send, y_recv, c_send, c_recv, r_send, r_recv, p_send, p_recv,
):
    me_x, me_y = lax.axis_index("gx"), lax.axis_index("gy")
    n_x, n_y = lax.axis_size("gx"), lax.axis_size("gy")

    def toward(r):
        dx, dy = OFFSETS[r]
        return (lax.rem(me_x + dx + n_x, n_x), lax.rem(me_y + dy + n_y, n_y))

    def remote(source, target, send, recv, r):
        return pltpu.make_async_remote_copy(
            src_ref=source, dst_ref=target, send_sem=send, recv_sem=recv,
            device_id=toward(r), device_id_type=pl.DeviceIdType.MESH,
        )

    load_vel = pltpu.make_async_copy(vel, block, local_sem.at[0])
    load_first = pltpu.make_async_copy(slots_h.at[:, pl.ds(0, MOVE)], first, local_sem.at[4])
    load_state = pltpu.make_async_copy(state, pool.at[pl.ds(0, SLOTS)], local_sem.at[1])
    load_slots = pltpu.make_async_copy(slots_h.at[:, pl.ds(0, MOVE)], slots, local_sem.at[5])
    load_cells = pltpu.make_async_copy(cells_h, cells, local_sem.at[6])
    for load in (load_vel, load_first, load_state, load_slots, load_cells):
        load.start()

    barrier = pltpu.get_barrier_semaphore()
    for r in range(8):
        pl.semaphore_signal(barrier, inc=1, device_id=toward(r), device_id_type=pl.DeviceIdType.MESH)
    load_vel.wait()
    faces[0] = edges(block, 0)
    faces[1] = edges(block, 15)
    for c in range(4):
        corners[c] = corner_rows(block, c)
    pl.semaphore_wait(barrier, 8)

    def rows_target(s, r):
        return landed.at[s, pl.ds((r ^ 1) * CAP, CAP)]

    def halo(s):
        part = pl.ds(s * 3, 3)
        copies = []
        for side, x, r in ((1, 0, 1), (0, 15, 0)):
            copies.append(remote(block.at[part, x], halo_x.at[side, part], x_send.at[s, side], x_recv.at[s, side], r))
        for side, edge, r in ((1, 0, 3), (0, 1, 2)):
            copies.append(remote(faces.at[edge, part], halo_y.at[side, part], y_send.at[s, side], y_recv.at[s, side], r))
        return copies

    corner_copies = [
        remote(corners.at[c], halo_c.at[3 - c], c_send.at[c], c_recv.at[3 - c], r)
        for c, r in ((0, 5), (1, 7), (2, 6), (3, 4))
    ]
    halos = [halo(s) for s in range(3)]
    row_copies = [
        [
            remote(rows.at[s, pl.ds(r * CAP, CAP)], rows_target(s, r), r_send.at[s, r], r_recv.at[s, r ^ 1], r)
            for r in range(8)
        ]
        for s in range(3)
    ]
    pv_copies = [
        [remote(out_pv.at[s, r // 2], in_pv.at[s, r ^ 1], p_send.at[s, r], p_recv.at[s, r ^ 1], r) for r in range(8)]
        for s in range(3)
    ]
    for copy in halos[0] + corner_copies:
        copy.start()
    load_first.wait()
    load_state.wait()
    copy_rows(rows.at[0], pool, lambda g, u: first[0, g * 128 + u], row_copies[0])
    for copy in halos[1] + halos[2]:
        copy.start()
    for b in range(16):
        pv[:, b * 128 : (b + 1) * 128] = pool[b * 128 : (b + 1) * 128, :].T[0:8, :]
    load_slots.wait()
    tables(counts, slots, ptr, dst, home, tail, filled)
    load_later = pltpu.make_async_copy(ptr, later, local_sem.at[7])
    load_later.start()
    for s in range(3):
        for k in range(3):
            own = block[s * 3 + k].reshape(256, 128)
            field[s, k * 256 : (k + 1) * 256, 0:128] = own
            field[s, k * 256 : (k + 1) * 256, 128:256] = own
    load_cells.wait()
    load_later.wait()

    def both(target, value):
        target[:, 0:128] = value
        target[:, 128:256] = value

    def place_halo(s):
        for copy in halos[s]:
            copy.wait_recv()
        for side in range(2):
            both(field.at[s, pl.ds(768 + side * 48, 48)], halo_x[side, s * 3 : s * 3 + 3].reshape(48, 128))
            both(field.at[s, pl.ds(864 + side * 48, 48)], halo_y[side, s * 3 : s * 3 + 3].reshape(48, 128))
        for c in range(4):
            both(field.at[s, pl.ds(960 + c * 16, 16)], halo_c[c])

    def advance(s, part, table, old, cell):
        fx, fy, fz = old[0:1], old[1:2], old[2:3]
        cx, cy, cz = cell
        near_hi, near_lo = split(1.0 - fz)
        far_hi, far_lo = split(fz)
        level = iota((128, CHUNK), 0)
        near = level == cz
        far = level == cz + 1
        weight = jnp.concatenate(
            [
                jnp.where(near, near_hi, jnp.where(far, far_hi, 0.0)).astype(BF16),
                jnp.where(near, near_lo, jnp.where(far, far_lo, 0.0)).astype(BF16),
            ],
            axis=0,
        )
        part[...] = jnp.dot(field[s], weight, preferred_element_type=F32)
        spot = iota((16, CHUNK), 0)
        wx = jnp.where(spot == cx, 1.0 - fx, jnp.where(spot == cx + 1, fx, 0.0))
        wy = jnp.where(spot == cy, 1.0 - fy, jnp.where(spot == cy + 1, fy, 0.0))
        table[...] = wx
        wx_low = jnp.where(cx == -1, 1.0 - fx, 0.0)
        wx_high = jnp.where(cx == 15, fx, 0.0)
        wy_low = jnp.where(cy == -1, 1.0 - fy, 0.0)
        wy_high = jnp.where(cy == 15, fy, 0.0)
        corner = jnp.zeros((16, CHUNK), F32)
        for c, w in enumerate((wx_low * wy_low, wx_low * wy_high, wx_high * wy_low, wx_high * wy_high)):
            corner = corner + part[960 + c * 16 : 976 + c * 16, :] * w
        new = []
        speeds = []
        for k in range(3):
            along = part[768 + k * 16 : 784 + k * 16, :] * wx_low + part[816 + k * 16 : 832 + k * 16, :] * wx_high
            for x in range(16):
                along = along + part[k * 256 + x * 16 : k * 256 + x * 16 + 16, :] * table[x : x + 1, :]
            edge = part[864 + k * 16 : 880 + k * 16, :] * wy_low + part[912 + k * 16 : 928 + k * 16, :] * wy_high
            total = along * wy + edge * wx + jnp.where(spot == s * 3 + k, corner, 0.0)
            speed = jnp.sum(total, axis=0, keepdims=True)
            speeds.append(speed)
            new.append(old[k : k + 1] + GAMMA[s] * speed + ZETA[s] * old[3 + k : 4 + k])
        return new + speeds

    def interpolate(s):
        def chunk(i, carry):
            at = pl.ds(pl.multiple_of(i * CHUNK, CHUNK), CHUNK)
            cell = [cells[s, c : c + 1, at] for c in range(3)]
            for k, value in enumerate(advance(s, sums.at[0], wx_table.at[0], pv[:, at], cell)):
                pv[k : k + 1, at] = value
            return carry

        lax.fori_loop(0, SLOTS // CHUNK, chunk, 0)

    def pick(s, take, zero):
        picked = []
        for g in range(4):
            q = slots[s : s + 1, g * 128 : (g + 1) * 128]
            low = jnp.broadcast_to(q & 127, (8, 128))
            high = jnp.broadcast_to(q >> 7, (8, 128))
            value = zero
            for h in range(16):
                value = jnp.where(high == h, lane_gather(take(slice(h * 128, (h + 1) * 128)), low), value)
            picked.append(value)
        return picked

    def collect_cells(s):
        def packed(at):
            one = (cells[s, 0:1, at] + 1) * 4096 + (cells[s, 1:2, at] + 1) * 128 + cells[s, 2:3, at]
            return jnp.broadcast_to(one, (8, 128))

        for g, value in enumerate(pick(s, packed, jnp.zeros((8, 128), I32))):
            one = value[0:1]
            at = slice(g * 128, (g + 1) * 128)
            away[s, 0:1, at] = (one >> 12) - 1
            away[s, 1:2, at] = ((one >> 7) & 31) - 1
            away[s, 2:3, at] = one & 127

    def collect(s):
        old = jnp.concatenate(pick(s, lambda at: pv[:, at], jnp.zeros((8, 128), F32)), axis=1)
        cell = [away[s, c : c + 1, :] for c in range(3)]
        new = advance(s, sums.at[1], wx_table.at[1], old, cell)
        for g in range(4):
            at = slice(g * 128, (g + 1) * 128)
            out_pv[s, g] = old[:, at]
            for k in range(6):
                out_pv[s, g, k : k + 1, :] = new[k][:, at]

    def deliver(s):
        lane = iota((8, 128), 1)
        came = [jnp.where(lane < CAP, in_pv[s, 2 * g + 1], in_pv[s, 2 * g]) for g in range(4)]
        value = jnp.concatenate(came, axis=1)
        high, rest = split(value)
        middle, low = split(rest)
        to = home[s : s + 1, :]
        parts = [jnp.where(to == h, part, 0.0).astype(BF16) for part in (high, middle, low) for h in range(16)]
        spread = rows_dot(jnp.concatenate(parts, axis=0), tail[s])
        for h in range(16):
            at = slice(h * 128, (h + 1) * 128)
            r = h * 8
            new = spread[r : r + 8] + spread[128 + r : 136 + r] + spread[256 + r : 264 + r]
            pv[:, at] = jnp.where(filled[s, h : h + 1, :] > 0.5, new, pv[:, at])

    for s in range(3):
        collect_cells(s)
    for copy in corner_copies:
        copy.wait_recv()
    stores = []
    for s in range(3):
        place_halo(s)
        collect(s)
        for copy in pv_copies[s]:
            copy.start()
        interpolate(s)
        for copy in row_copies[s]:
            copy.wait_recv()
        store = pltpu.make_async_copy(landed.at[s], rows_out.at[pl.ds(s * MOVE, MOVE)], local_sem.at[8 + s])
        store.start()
        stores.append(store)
        if s < 2:
            pool[SLOTS + s * MOVE : SLOTS + (s + 1) * MOVE, :] = landed[s]
            copy_rows(rows.at[s + 1], pool, lambda g, u: later[s * 4 + g, u], row_copies[s + 1])
        for copy in pv_copies[s]:
            copy.wait_recv()
        deliver(s)
    pv_out[...] = pv[...]
    for store in stores:
        store.wait()
    for copies in halos + [corner_copies] + row_copies + pv_copies:
        for copy in copies:
            copy.wait_send()


def finish_kernel(dst_h, state, rows_h, pv_h, out, held, rows, pv, dst, sem, out_sem):
    loads = [
        pltpu.make_async_copy(state, held.at[pl.ds(0, SLOTS)], sem.at[0]),
        pltpu.make_async_copy(dst_h, dst, sem.at[1]),
        pltpu.make_async_copy(rows_h, rows, sem.at[2]),
        pltpu.make_async_copy(pv_h, pv, sem.at[3]),
    ]
    for load in loads:
        load.start()
    for load in loads:
        load.wait()

    def body(g, carry):
        for u in range(128):
            held[pl.ds(dst[g, u], 1), :] = rows[pl.ds(g * 128 + u, 1), :]
        return carry

    lax.fori_loop(0, 12, body, 0)
    stores = []
    for c in range(4):
        for b in range(c * 4, c * 4 + 4):
            held[b * 128 : (b + 1) * 128, 0:8] = pv[:, b * 128 : (b + 1) * 128].T
        part = pl.ds(c * 512, 512)
        stores.append(pltpu.make_async_copy(held.at[part], out.at[part], out_sem.at[c]))
        stores[-1].start()
    for store in stores:
        store.wait()


def whole(space):
    return pl.BlockSpec(memory_space=space)


def shape(dims, dtype):
    return jax.ShapeDtypeStruct(dims, dtype)


def local(state, velocity, cells, slots, counts):
    dma = pltpu.SemaphoreType.DMA
    pv, rows, dst = pl.pallas_call(
        step_kernel,
        out_shape=(shape((8, SLOTS), F32), shape((3 * MOVE, 128), F32), shape((12, 128), I32)),
        in_specs=[whole(SMEM)] + [whole(ANY)] * 4,
        out_specs=[whole(VMEM), whole(ANY), whole(VMEM)],
        scratch_shapes=[
            VMEM((SLOTS + 2 * MOVE, 128), F32),
            VMEM((3, MOVE, 128), F32),
            VMEM((3, MOVE, 128), F32),
            VMEM((9, 16, 16, 128), BF16),
            VMEM((2, 9, 16, 128), BF16),
            VMEM((4, 16, 128), BF16),
            VMEM((2, 9, 16, 128), BF16),
            VMEM((2, 9, 16, 128), BF16),
            VMEM((4, 16, 128), BF16),
            VMEM((3, 1024, 256), BF16),
            VMEM((2, 16, CHUNK), F32),
            VMEM((2, 1024, CHUNK), F32),
            VMEM((8, SLOTS), F32),
            VMEM((3, 4, 8, 128), F32),
            VMEM((3, 8, 8, 128), F32),
            VMEM((3, 3, SLOTS), I32),
            VMEM((3, 8, MOVE), I32),
            VMEM((3, MOVE), I32),
            VMEM((3, MOVE), I32),
            VMEM((3, 128, MOVE), BF16),
            VMEM((3, 16, 128), F32),
            VMEM((8, 128), I32),
            SMEM((3, MOVE), I32),
            SMEM((8, 128), I32),
            dma((11,)),
            dma((3, 2)), dma((3, 2)), dma((3, 2)), dma((3, 2)),
            dma((4,)), dma((4,)),
            dma((3, 8)), dma((3, 8)), dma((3, 8)), dma((3, 8)),
        ],
        compiler_params=pltpu.CompilerParams(collective_id=0, has_side_effects=True),
        name="step",
    )(counts, cells, slots, state, velocity.reshape(9, 16, 16, 128))

    return pl.pallas_call(
        finish_kernel,
        out_shape=shape((SLOTS, 128), F32),
        in_specs=[whole(ANY)] * 4,
        out_specs=whole(ANY),
        scratch_shapes=[
            VMEM((SLOTS + 8, 128), F32),
            VMEM((3 * MOVE, 128), F32),
            VMEM((8, SLOTS), F32),
            SMEM((12, 128), I32),
            dma((4,)),
            dma((4,)),
        ],
        name="finish",
    )(dst, state, rows, pv)


def solution(mesh):
    return jax.shard_map(
        local,
        mesh=mesh,
        in_specs=(
            P(("gx", "gy"), None),
            P(None, None, "gx", "gy", None),
            P(None, None, ("gx", "gy")),
            P(None, ("gx", "gy")),
            P(None, "gx", "gy", None),
        ),
        out_specs=P(("gx", "gy"), None),
        check_vma=False,
    )
```
